32 devices in a mesh: seq: 8 (over z, x), head: 2 (over y), batch: 2 (over core).
Axes of the slice: x: 2, y: 2, z: 4, core: 2. Of those that a mesh axis runs over, the one named last changes fastest.
Arguments:
- queries: bfloat16 [2, 4096, 32, 128], P('batch', 'seq', 'head'), may hold values from -200 to 200
- key_states: bfloat16 [2, 4096, 8, 128], P('batch', 'seq', 'head'), may hold values from -7 to 7
- value_vectors: bfloat16 [2, 4096, 8, 128], P('batch', 'seq', 'head'), may hold values from -6 to 6
- block_doc: int32 [2, 32], P('batch'), may hold values from 0 to 7, never falling along the last dimension, each value on 1 to 20 neighbouring positions
- out_weight: bfloat16 [4096, 8192], P('head', 'batch'), may hold values from -0.5 to 0.5
Outputs:
- projected: bfloat16 [4096, 2, 8192], P(('seq', 'head'), None, 'batch')
The draws below stay inside these ranges and needn't reach their ends.
Inputs may be any that keep to these rules, and one draw needn't show every extreme that they name: block_doc[b, j] never falls along j, starts at 0 and skips no number; every document covers 1 to 20 whole blocks, and some document covers exactly 20.
All inputs are finite; a program needn't handle non-finite values.
Results may differ from the reference program's by a relative error of at most 0.0095.
Values may be sent and summed in bfloat16 or wider, within the bound.
A program may use at most 128 MiB of HBM per device.

```python
import math
import jax
import jax.numpy as jnp
import numpy as np
from jax import lax

D = 8192
QUERY_HEADS = 32
KEY_VALUE_HEADS = 8
HEAD_WIDTH = 128
BLK = 128
SEQUENCE_LENGTH = 4096
PACKED_BATCH = 2
NBLK = 32
MOSTB = 20
NDOC = 8
HQ_DEV = 16
HGROUPS = 2


def draw_pair(key):
    query_draw = jax.random.normal(jax.random.fold_in(key, 11), (PACKED_BATCH, SEQUENCE_LENGTH, QUERY_HEADS, HEAD_WIDTH), jnp.float32)
    key_sample = jnp.clip(jax.random.normal(jax.random.fold_in(key, 12), (PACKED_BATCH, SEQUENCE_LENGTH, KEY_VALUE_HEADS, HEAD_WIDTH), jnp.float32), -6.0, 6.0)
    query_draw = jnp.clip(query_draw, -6.0, 6.0)
    return (query_draw, key_sample)


def draw_queries(key, part):
    return draw_pair(key)[0].astype(jnp.bfloat16)


def draw_key_states(key, part):
    return draw_pair(key)[1].astype(jnp.bfloat16)


def shard_levels(stream_key, extent, cuts, low, top_value):
    loudness, own = 1.0, jax.random.fold_in(stream_key, 6)
    for dim, blocks in cuts:
        heights = jnp.exp(jax.random.uniform(jax.random.fold_in(own, dim), (blocks,), jnp.float32, low / len(cuts), top_value / len(cuts)))
        loudness = loudness * jnp.repeat(heights, extent[dim] // blocks).reshape([-1 if axis == dim else 1 for axis in range(len(extent))])
    return loudness


def profile(count, total, limit, slope):
    weights = [(1 << 20) // math.isqrt(grade ** slope) + 1 for grade in range(2, count + 1)]
    rest, given = total - limit - (count - 1), [1] * (count - 1)
    while rest > 0:
        free = [i for i in range(count - 1) if given[i] < limit]
        pool, budget = sum([weights[i] for i in free]), rest
        for i in free:
            addition = min(limit - given[i], max(1, budget * weights[i] // pool), rest)
            given[i] = given[i] + addition
            rest = rest - addition
    return np.array([limit] + given)


def ragged_sizes(key, amount, total, limit, lean):
    if amount == 2:
        one = jax.random.randint(key, (), max(1, total - limit), min(limit, total - 1) + 1)
        return jnp.stack([one, total - one])
    tallies = jnp.asarray(profile(amount, total, limit, lean), jnp.int32)
    pairs = (amount - 1) // 2
    source_of, receiver = tallies[1:1 + 2 * pairs:2], tallies[2:2 + 2 * pairs:2]
    slack = jnp.minimum(source_of - 1, limit - receiver)
    moved = jax.random.randint(jax.random.fold_in(key, 1), (pairs,), 0, 1 << 20) % (slack + 1)
    tallies = tallies.at[1:1 + 2 * pairs:2].set(source_of - moved).at[2:2 + 2 * pairs:2].set(receiver + moved)
    return tallies[jax.random.permutation(jax.random.fold_in(key, 2), amount)]


def gaussian(key, shape, spread, most, split=(), kind=jnp.bfloat16):
    drawn = spread * jax.random.normal(key, shape, jnp.float32)
    if split:
        drawn = drawn * shard_levels(key, shape, split, -0.22, 0.18)
    return jnp.clip(drawn, -most, most).astype(kind)


def setup_inputs(seed: int = 0) -> dict:
    streams_of = jax.random.split(jax.random.key(seed), 6)
    queries = draw_queries(jax.random.fold_in(streams_of[5], 71), 0)
    key_states = draw_key_states(jax.random.fold_in(streams_of[5], 71), 0)
    value_vectors = gaussian(streams_of[2], (PACKED_BATCH, SEQUENCE_LENGTH, KEY_VALUE_HEADS, HEAD_WIDTH), 1.0, 6.0, ((0, 2), (1, 8), (2, 2)))
    block_doc = jax.vmap(lambda own: jnp.searchsorted(jnp.cumsum(ragged_sizes(own, NDOC, NBLK, MOSTB, 2)), jnp.arange(NBLK), side="right"))(jax.random.split(streams_of[3], PACKED_BATCH)).reshape((PACKED_BATCH, NBLK)).astype(jnp.int32)
    out_weight = gaussian(streams_of[4], (QUERY_HEADS * HEAD_WIDTH, D), HEAD_WIDTH ** -0.5, 0.5, ((0, 2), (1, 2)))
    return {"queries": queries, "key_states": key_states, "value_vectors": value_vectors, "block_doc": block_doc, "out_weight": out_weight}


def reference(queries, key_states, value_vectors, block_doc, out_weight):
    group_count_per_key = QUERY_HEADS // KEY_VALUE_HEADS
    score_scale = HEAD_WIDTH ** -0.5
    positions = jnp.arange(SEQUENCE_LENGTH, dtype=jnp.int32)
    results = []
    for batch_index in range(PACKED_BATCH):
        doc_tok = jnp.repeat(block_doc[batch_index], BLK)
        visible = (doc_tok[:, None] == doc_tok[None, :]) & (positions[:, None] >= positions[None, :])
        query_seq = queries[batch_index]
        key_seq = key_states[batch_index]
        value_seq = value_vectors[batch_index]

        def head_out(head_index):
            q_head = lax.dynamic_index_in_dim(query_seq, head_index, 1, False)
            k_head = lax.dynamic_index_in_dim(key_seq, head_index // group_count_per_key, 1, False)
            v_head = lax.dynamic_index_in_dim(value_seq, head_index // group_count_per_key, 1, False)
            scores = jnp.dot(q_head, k_head.T, preferred_element_type=jnp.float32) * score_scale
            scores = jnp.where(visible, scores, -1e30)
            maxima = jnp.max(scores, axis=1)
            weights = jnp.where(visible, jnp.exp(scores - maxima[:, None]), 0.0)
            denominator = jnp.sum(weights, axis=1)
            numerator = jnp.dot(weights.astype(jnp.bfloat16), v_head, preferred_element_type=jnp.float32)
            return (numerator / denominator[:, None]).astype(jnp.bfloat16)

        attended = lax.map(head_out, jnp.arange(QUERY_HEADS, dtype=jnp.int32))
        flattened = jnp.transpose(attended, (1, 0, 2)).reshape(SEQUENCE_LENGTH, QUERY_HEADS * HEAD_WIDTH)
        group_width = HQ_DEV * HEAD_WIDTH
        summed = jnp.zeros((SEQUENCE_LENGTH, D), jnp.float32)
        for group_index in range(HGROUPS):
            lower = group_index * group_width
            partial_value = jnp.dot(flattened[:, lower:lower + group_width], out_weight[lower:lower + group_width], preferred_element_type=jnp.float32).astype(jnp.bfloat16)
            partial_value = lax.optimization_barrier(partial_value)
            summed = summed + partial_value.astype(jnp.float32)
        results.append(summed.astype(jnp.bfloat16))
    return jnp.stack(results, axis=1)
```

```python
import functools
import math

import jax
import jax.numpy as jnp
from jax import lax
from jax.experimental import pallas as pl
from jax.experimental.pallas import tpu as pltpu
from jax.sharding import PartitionSpec as P


HIDDEN = -1e30


def move(block, axis, pairs):
    return jax.tree.map(lambda array: lax.ppermute(array, axis, pairs), block)


def gather_plan(span):
    plan = [("own", 0)]
    for k in range(1, span // 2 + 1):
        plan.append(("same", k))
    for k in range(0, (span + 1) // 2 + 1):
        if 2 * k + 1 <= span or 1 <= 2 * k - 1 <= span:
            plan.append(("cross", k))
    return plan


def gather_shards(own, plan, span, seq_count):
    positions = range(seq_count)
    same = {0: own}
    result = []
    for kind, k in plan:
        if kind == "same":
            same[k] = move(same[k - 1], "seq", [(s, s + 2) for s in positions if s + 2 < seq_count])
    for kind, k in plan:
        if kind != "cross":
            result.append(same[k])
        elif k in same:
            pairs = []
            for s in positions:
                to = s + 1 if s % 2 == 0 else s - 1
                distance = to - s + 2 * k
                if 0 < distance <= span and to - distance >= 0 and to < seq_count:
                    pairs.append((s, to))
            result.append(move(same[k], "seq", pairs))
        else:
            pairs = [(s, s + 2 * k - 1) for s in positions if s % 2 == 1 and s + 2 * k - 1 < seq_count]
            result.append(move(own, "seq", pairs))
    return result


def attention_kernel(plan, span, block_len, group, head_dim, kv_heads, info, q_ref, *rest):
    shards = list(zip(rest[: len(plan)], rest[len(plan) : 2 * len(plan)]))
    out_ref, keys, values, sems = rest[2 * len(plan) :]
    rows = shards[0][0].shape[0]
    head = pl.program_id(0)
    parity = info[0]
    first_key = info[1]
    q_row = info[2]

    @pl.when(head == 0)
    def _():
        def each(act):
            for i, (kind, k) in enumerate(plan):
                if kind == "cross":
                    distance = 2 * k - 1 + 2 * parity
                else:
                    distance = 2 * k
                at = pl.multiple_of((span - distance) * rows, rows)

                def both(i=i, at=at):
                    act(pltpu.make_async_copy(shards[i][0], keys.at[pl.ds(at, rows)], sems.at[i, 0]))
                    act(pltpu.make_async_copy(shards[i][1], values.at[:, pl.ds(at, rows)], sems.at[i, 1]))

                if kind == "cross":
                    pl.when((distance > 0) & (distance <= span))(both)
                else:
                    both()

        each(lambda copy: copy.start())
        each(lambda copy: copy.wait())

    chunk = 2 * block_len
    lanes = pl.ds(pl.multiple_of(head * head_dim, head_dim), head_dim)
    factor = math.log2(math.e) / math.sqrt(head_dim)
    q_all = q_ref[...]
    halves = 2
    per = group // halves
    width = per * block_len
    queries = [
        jnp.concatenate(
            [q_all[:, j * head_dim : (j + 1) * head_dim] for j in range(a * per, (a + 1) * per)], axis=0
        )
        for a in range(halves)
    ]
    last = span * rows + q_row + block_len

    def scores_of(begin, a):
        k_chunk = keys[pl.ds(begin, chunk), lanes]
        return lax.dot_general(
            k_chunk, queries[a], (((1,), (1,)), ((), ())), preferred_element_type=jnp.float32
        )

    def step(begin, state, first, masked):
        begin = pl.multiple_of(begin, block_len)
        v_chunk = values[lanes, pl.ds(begin, chunk)]
        done = []
        for a in range(halves):
            s = scores_of(begin, a)
            if masked:
                row = lax.broadcasted_iota(jnp.int32, (chunk, width), 0)
                hide = row < first_key - begin
                if first:
                    tok = lax.broadcasted_iota(jnp.int32, (chunk, width), 1) & (block_len - 1)
                    hide = hide | (row > tok + (chunk - block_len))
                s = jnp.where(hide, HIDDEN, s)
            top = jnp.max(s, axis=0, keepdims=True)
            if not first:
                top = jnp.maximum(top, state[a][0])
            p = jnp.exp2((s - top) * factor)
            total = jnp.sum(p, axis=0, keepdims=True)
            acc = jnp.dot(v_chunk, p.astype(jnp.bfloat16), preferred_element_type=jnp.float32)
            if not first:
                fade = jnp.exp2((state[a][0] - top) * factor)
                total = total + state[a][1] * fade
                acc = acc + state[a][2] * fade
            done.append((top, total, acc))
        return tuple(done)

    state = step(last - chunk, None, True, True)
    count = (last - first_key) // chunk
    spare = (last - first_key) - count * chunk

    def body(t, state):
        return step(last - (t + 1) * chunk, state, False, False)

    state = lax.fori_loop(1, count, body, state)
    state = lax.cond(
        (spare > 0) & (count > 0),
        lambda state: step(last - (count + 1) * chunk, state, False, True),
        lambda state: state,
        state,
    )
    pieces = []
    for a in range(halves):
        o = state[a][2] / state[a][1]
        for j in range(per):
            pieces.append(o[:, j * block_len : (j + 1) * block_len].T)
    out_ref[...] = jnp.concatenate(pieces, axis=1).astype(out_ref.dtype)


def attend(info, q_flat, shards, plan, span, block_len, kv_heads, group, head_dim):
    rows = shards[0][0].shape[0]
    wide = group * head_dim
    work = 2 * 2 * block_len * rows * 2 * kv_heads * group * head_dim
    return pl.pallas_call(
        functools.partial(attention_kernel, plan, span, block_len, group, head_dim, kv_heads),
        grid_spec=pltpu.PrefetchScalarGridSpec(
            num_scalar_prefetch=1,
            grid=(kv_heads,),
            in_specs=[pl.BlockSpec((block_len, wide), lambda h, info: (info[2] // block_len, h))]
            + [pl.BlockSpec(memory_space=pl.ANY)] * (2 * len(plan)),
            out_specs=pl.BlockSpec((block_len, wide), lambda h, info: (0, h)),
            scratch_shapes=[
                pltpu.VMEM(((span + 1) * rows, kv_heads * head_dim), jnp.bfloat16),
                pltpu.VMEM((kv_heads * head_dim, (span + 1) * rows), jnp.bfloat16),
                pltpu.SemaphoreType.DMA((len(plan), 2)),
            ],
        ),
        out_shape=jax.ShapeDtypeStruct((block_len, kv_heads * wide), jnp.bfloat16),
        compiler_params=pltpu.CompilerParams(dimension_semantics=("arbitrary",)),
        cost_estimate=pl.CostEstimate(
            flops=work, bytes_accessed=4 * (span + 1) * rows * kv_heads * head_dim, transcendentals=0
        ),
    )(info, q_flat, *[k for k, _ in shards], *[v for _, v in shards])


def on_device(queries, key_states, value_vectors, block_doc, out_weight):
    tok_rows, q_heads, head_dim = queries.shape[1:]
    kv_heads = key_states.shape[2]
    group = q_heads // kv_heads
    blocks_total = block_doc.shape[1]
    seq_count = lax.axis_size("seq")
    heads_count = lax.axis_size("head")
    batch_count = lax.axis_size("batch")
    block_len = tok_rows * seq_count // blocks_total
    seq_index = lax.axis_index("seq")
    head_index = lax.axis_index("head")
    batch_index = lax.axis_index("batch")
    blocks_dev = tok_rows // block_len
    longest = blocks_total // 2 + blocks_dev
    longest = longest + longest % 2
    span = (longest + blocks_dev - 2) // blocks_dev

    own = (
        key_states[0].reshape(tok_rows, kv_heads * head_dim),
        value_vectors[0].reshape(tok_rows, kv_heads * head_dim).T,
    )
    plan = gather_plan(span)
    shards = gather_shards(own, plan, span, seq_count)
    q_flat = queries[0].reshape(tok_rows, q_heads * head_dim)

    docs = block_doc[0]
    own_docs = lax.dynamic_slice_in_dim(docs, seq_index * blocks_dev, blocks_dev)
    first_block = jnp.sum((docs[None, :] < own_docs[:, None]).astype(jnp.int32), axis=1)
    first_key = (first_block - (seq_index - span) * blocks_dev) * block_len

    part_rows = tok_rows // heads_count
    part_blocks = part_rows // block_len
    ring = range(batch_count)

    def attended_of(hop, b, after):
        block = lax.rem(head_index + hop, heads_count) * part_blocks + b
        info = jnp.stack([seq_index % 2, first_key[block], block * block_len]).astype(jnp.int32)
        if after is not None:
            info, _ = lax.optimization_barrier((info, after))
        mine = attend(info, q_flat, shards, plan, span, block_len, kv_heads, group, head_dim)
        return [mine] + [move(mine, "batch", [(i, (i + turn) % batch_count) for i in ring]) for turn in range(1, batch_count)]

    def project(rows, after):
        if after is not None:
            rows, _ = lax.optimization_barrier((rows, after))
        return jnp.dot(rows, out_weight, preferred_element_type=jnp.float32).astype(jnp.bfloat16)

    steps = [(hop, b) for hop in list(range(1, heads_count)) + [0] for b in range(part_blocks)]
    terms = [[[] for _ in ring] for _ in range(part_blocks)]
    after = None
    for hop, b in steps:
        for turn, rows in enumerate(attended_of(hop, b, after)):
            after = project(rows, after)
            partial = after
            if hop:
                partial = move(after, "head", [(i, (i + hop) % heads_count) for i in range(heads_count)])
            terms[b][turn].append(partial)
    done = []
    for b in range(part_blocks):
        turns = []
        for turn in ring:
            parts, _ = lax.optimization_barrier((terms[b][turn], after))
            turns.append(sum(part.astype(jnp.float32) for part in parts).astype(jnp.bfloat16))
        ordered = []
        for n in ring:
            picked = turns[0]
            for turn in range(1, batch_count):
                picked = jnp.where(lax.rem(batch_index - turn + batch_count, batch_count) == n, turns[turn], picked)
            ordered.append(picked)
        done.append(jnp.stack(ordered, axis=1))
    return jnp.concatenate(done, axis=0)


def solution(mesh):
    return jax.shard_map(
        on_device,
        mesh=mesh,
        in_specs=(
            P("batch", "seq", "head", None),
            P("batch", "seq", "head", None),
            P("batch", "seq", "head", None),
            P("batch", None),
            P("head", "batch"),
        ),
        out_specs=P(("seq", "head"), None, "batch"),
        check_vma=False,
    )
```

```python
import functools
import math

import jax
import jax.numpy as jnp
from jax import lax
from jax.experimental import pallas as pl
from jax.experimental.pallas import tpu as pltpu
from jax.sharding import PartitionSpec as P


HIDDEN = -1e30


def move(block, axis, pairs):
    return jax.tree.map(lambda array: lax.ppermute(array, axis, pairs), block)


def gather_plan(span):
    plan = [("own", 0)]
    for k in range(1, span // 2 + 1):
        plan.append(("same", k))
    for k in range(0, (span + 1) // 2 + 1):
        if 2 * k + 1 <= span or 1 <= 2 * k - 1 <= span:
            plan.append(("cross", k))
    return plan


def gather_shards(own, plan, span, seq_count):
    positions = range(seq_count)
    same = {0: own}
    result = []
    for kind, k in plan:
        if kind == "same":
            same[k] = move(same[k - 1], "seq", [(s, s + 2) for s in positions if s + 2 < seq_count])
    for kind, k in plan:
        if kind != "cross":
            result.append(same[k])
        elif k in same:
            pairs = []
            for s in positions:
                to = s + 1 if s % 2 == 0 else s - 1
                distance = to - s + 2 * k
                if 0 < distance <= span and to - distance >= 0 and to < seq_count:
                    pairs.append((s, to))
            result.append(move(same[k], "seq", pairs))
        else:
            pairs = [(s, s + 2 * k - 1) for s in positions if s % 2 == 1 and s + 2 * k - 1 < seq_count]
            result.append(move(own, "seq", pairs))
    return result


def attention_kernel(plan, span, block_len, group, head_dim, info, q_ref, *rest):
    shards = list(zip(rest[: len(plan)], rest[len(plan) : 2 * len(plan)]))
    out_ref, keys, values, sems = rest[2 * len(plan) :]
    rows = shards[0][0].shape[0]
    head = pl.program_id(0)
    parity = info[0]
    first_key = info[1]
    q_row = info[2]

    @pl.when(head == 0)
    def _():
        def each(act):
            for i, (kind, k) in enumerate(plan):
                if kind == "cross":
                    distance = 2 * k - 1 + 2 * parity
                else:
                    distance = 2 * k
                at = pl.multiple_of((span - distance) * rows, rows)

                def both(i=i, at=at):
                    act(pltpu.make_async_copy(shards[i][0], keys.at[pl.ds(at, rows)], sems.at[i, 0]))
                    act(pltpu.make_async_copy(shards[i][1], values.at[:, pl.ds(at, rows)], sems.at[i, 1]))

                if kind == "cross":
                    pl.when((distance > 0) & (distance <= span))(both)
                else:
                    both()

        each(lambda copy: copy.start())
        each(lambda copy: copy.wait())

    chunk = 2 * block_len
    lanes = pl.ds(pl.multiple_of(head * head_dim, head_dim), head_dim)
    factor = math.log2(math.e) / math.sqrt(head_dim)
    q_all = q_ref[...]
    halves = 2
    per = group // halves
    width = per * block_len
    queries = [
        jnp.concatenate(
            [q_all[:, j * head_dim : (j + 1) * head_dim].T for j in range(a * per, (a + 1) * per)], axis=1
        )
        for a in range(halves)
    ]
    last = span * rows + q_row + block_len

    def scores_of(begin, a):
        k_chunk = keys[pl.ds(begin, chunk), lanes]
        return jnp.dot(k_chunk, queries[a], preferred_element_type=jnp.float32)

    def step(begin, state, first, masked):
        begin = pl.multiple_of(begin, block_len)
        v_chunk = values[lanes, pl.ds(begin, chunk)]
        done = []
        for a in range(halves):
            s = scores_of(begin, a)
            if masked:
                row = lax.broadcasted_iota(jnp.int32, (chunk, width), 0)
                hide = row < first_key - begin
                if first:
                    tok = lax.broadcasted_iota(jnp.int32, (chunk, width), 1) & (block_len - 1)
                    hide = hide | (row > tok + (chunk - block_len))
                s = jnp.where(hide, HIDDEN, s)
            top = jnp.max(s, axis=0, keepdims=True)
            if not first:
                top = jnp.maximum(top, state[a][0])
            p = jnp.exp2((s - top) * factor)
            total = jnp.sum(p, axis=0, keepdims=True)
            acc = jnp.dot(v_chunk, p.astype(jnp.bfloat16), preferred_element_type=jnp.float32)
            if not first:
                fade = jnp.exp2((state[a][0] - top) * factor)
                total = total + state[a][1] * fade
                acc = acc + state[a][2] * fade
            done.append((top, total, acc))
        return tuple(done)

    state = step(last - chunk, None, True, True)
    count = (last - first_key) // chunk
    spare = (last - first_key) - count * chunk

    def body(t, state):
        return step(last - (t + 1) * chunk, state, False, False)

    state = lax.fori_loop(1, count, body, state)
    state = lax.cond(
        (spare > 0) & (count > 0),
        lambda state: step(last - (count + 1) * chunk, state, False, True),
        lambda state: state,
        state,
    )
    pieces = []
    for a in range(halves):
        o = state[a][2] / state[a][1]
        for j in range(per):
            pieces.append(o[:, j * block_len : (j + 1) * block_len].T)
    out_ref[...] = jnp.concatenate(pieces, axis=1).astype(out_ref.dtype)


def attend(info, q_flat, shards, plan, span, block_len, kv_heads, group, head_dim):
    rows = shards[0][0].shape[0]
    wide = group * head_dim
    work = 2 * 2 * block_len * rows * 2 * kv_heads * group * head_dim
    return pl.pallas_call(
        functools.partial(attention_kernel, plan, span, block_len, group, head_dim),
        grid_spec=pltpu.PrefetchScalarGridSpec(
            num_scalar_prefetch=1,
            grid=(kv_heads,),
            in_specs=[pl.BlockSpec((block_len, wide), lambda h, info: (info[2] // block_len, h))]
            + [pl.BlockSpec(memory_space=pl.ANY)] * (2 * len(plan)),
            out_specs=pl.BlockSpec((block_len, wide), lambda h, info: (0, h)),
            scratch_shapes=[
                pltpu.VMEM(((span + 1) * rows, kv_heads * head_dim), jnp.bfloat16),
                pltpu.VMEM((kv_heads * head_dim, (span + 1) * rows), jnp.bfloat16),
                pltpu.SemaphoreType.DMA((len(plan), 2)),
            ],
        ),
        out_shape=jax.ShapeDtypeStruct((block_len, kv_heads * wide), jnp.bfloat16),
        compiler_params=pltpu.CompilerParams(dimension_semantics=("arbitrary",)),
        cost_estimate=pl.CostEstimate(
            flops=work, bytes_accessed=4 * (span + 1) * rows * kv_heads * head_dim, transcendentals=0
        ),
    )(info, q_flat, *[k for k, _ in shards], *[v for _, v in shards])


def on_device(queries, key_states, value_vectors, block_doc, out_weight):
    tok_rows, q_heads, head_dim = queries.shape[1:]
    kv_heads = key_states.shape[2]
    group = q_heads // kv_heads
    blocks_total = block_doc.shape[1]
    seq_count = lax.axis_size("seq")
    heads_count = lax.axis_size("head")
    batch_count = lax.axis_size("batch")
    block_len = tok_rows * seq_count // blocks_total
    seq_index = lax.axis_index("seq")
    head_index = lax.axis_index("head")
    batch_index = lax.axis_index("batch")
    blocks_dev = tok_rows // block_len
    longest = blocks_total // 2 + blocks_dev
    longest = longest + longest % 2
    span = (longest + blocks_dev - 2) // blocks_dev

    own = (
        key_states[0].reshape(tok_rows, kv_heads * head_dim),
        value_vectors[0].reshape(tok_rows, kv_heads * head_dim).T,
    )
    plan = gather_plan(span)
    shards = gather_shards(own, plan, span, seq_count)
    q_flat = queries[0].reshape(tok_rows, q_heads * head_dim)

    docs = block_doc[0]
    own_docs = lax.dynamic_slice_in_dim(docs, seq_index * blocks_dev, blocks_dev)
    first_block = jnp.sum((docs[None, :] < own_docs[:, None]).astype(jnp.int32), axis=1)
    first_key = (first_block - (seq_index - span) * blocks_dev) * block_len

    part_rows = tok_rows // heads_count
    part_blocks = part_rows // block_len
    ring = range(batch_count)

    def attended_of(hop, b, after):
        block = lax.rem(head_index + hop, heads_count) * part_blocks + b
        info = jnp.stack([seq_index % 2, first_key[block], block * block_len]).astype(jnp.int32)
        if after is not None:
            info, _ = lax.optimization_barrier((info, after))
        mine = attend(info, q_flat, shards, plan, span, block_len, kv_heads, group, head_dim)
        return [mine] + [move(mine, "batch", [(i, (i + turn) % batch_count) for i in ring]) for turn in range(1, batch_count)]

    def project(rows, after):
        if after is not None:
            rows, _ = lax.optimization_barrier((rows, after))
        return jnp.dot(rows, out_weight, preferred_element_type=jnp.float32).astype(jnp.bfloat16)

    steps = [(hop, b) for hop in list(range(1, heads_count)) + [0] for b in range(part_blocks)]
    terms = [[[] for _ in ring] for _ in range(part_blocks)]
    after = None
    kept = []
    for hop, b in steps:
        rows = attended_of(hop, b, after)
        if not hop:
            kept = kept + rows
            continue
        after = project(jnp.concatenate(rows, axis=0), after)
        partial = move(after, "head", [(i, (i + hop) % heads_count) for i in range(heads_count)])
        for turn, piece in enumerate(jnp.split(partial, batch_count)):
            terms[b][turn].append(piece)
    after = project(jnp.concatenate(kept, axis=0), after)
    for at, piece in enumerate(jnp.split(after, len(kept))):
        terms[at // batch_count][at % batch_count].append(piece)
    done = []
    for b in range(part_blocks):
        turns = []
        for turn in ring:
            parts, _ = lax.optimization_barrier((terms[b][turn], after))
            turns.append(sum(part.astype(jnp.float32) for part in parts).astype(jnp.bfloat16))
        ordered = []
        for n in ring:
            picked = turns[0]
            for turn in range(1, batch_count):
                picked = jnp.where(lax.rem(batch_index - turn + batch_count, batch_count) == n, turns[turn], picked)
            ordered.append(picked)
        done.append(jnp.stack(ordered, axis=1))
    return jnp.concatenate(done, axis=0)


def solution(mesh):
    return jax.shard_map(
        on_device,
        mesh=mesh,
        in_specs=(
            P("batch", "seq", "head", None),
            P("batch", "seq", "head", None),
            P("batch", "seq", "head", None),
            P("batch", None),
            P("head", "batch"),
        ),
        out_specs=P(("seq", "head"), None, "batch"),
        check_vma=False,
    )
```
